256 devices in a mesh: dp: 32 (over y, z_lo, x), tensor: 8 (over z_hi, core).
Axes of the slice: x: 4, y: 4, z: 8 (z_hi: 4, z_lo: 2; z = z_hi * 2 + z_lo), core: 2. Of those that a mesh axis runs over, the one named last changes fastest.
Arguments:
- hidden: bfloat16 [32768, 7168], P('dp', 'tensor'), parts along dimension 0, may hold values from -6 to 6
- w_dq: bfloat16 [7168, 1536], P('tensor'), may hold values from -0.0625 to 0.0625
- w_dkv: bfloat16 [7168, 576], P('tensor'), may hold values from -0.0625 to 0.0625
- q_gain: float32 [1536], replicated, may hold values from 0.1 to 1.9
- kv_gain: float32 [512], replicated, may hold values from 0.1 to 1.9
- w_uq: bfloat16 [1536, 12288], P(None, 'tensor'), may hold values from -0.15625 to 0.15625
- w_ukv: bfloat16 [512, 16384], P(None, 'tensor'), may hold values from -0.25 to 0.25
Outputs:
- queries: bfloat16 [32768, 12288], P('dp', 'tensor'), parts along dimension 0
- keys_values: bfloat16 [32768, 16384], P('dp', 'tensor'), parts along dimension 0
- rotary_key: bfloat16 [32768, 64], P(('dp', 'tensor')), parts along dimension 0
The draws below stay inside these ranges and needn't reach their ends.
There are 32 independent parts, one for each index of `dp`. The reference program is written for one: setup_inputs(seed, part) draws one part's arguments, and reference() takes and returns one part's arrays. A program takes and returns all parts, laid end to end along the dimension named above; an argument that names none is the same for every part. Nothing has to cross between parts.
All inputs are finite; a program needn't handle non-finite values.
Results may differ from the reference program's by a relative error of at most 0.0049.
Values may be sent and summed in bfloat16 or wider, within the bound.
No kernel may reach another device: no remote copies, remote signals or barrier semaphores. Data moves between devices by JAX's collectives and lax.ppermute only.
A program may use at most 128 MiB of HBM per device.

```python
import jax
import jax.numpy as jnp
from jax import lax

D = 7168
QL = 1536
KL = 512
HEADS = 64
NOPE = 128
ROPE = 64
VDIM = 128
TOK = 1024


def block_scale(own_key, shape, split, least, top_value):
    level = 1.0
    for dim, shards_of in split:
        draws = jax.random.uniform(jax.random.fold_in(jax.random.fold_in(own_key, 6), dim), (shards_of,), jnp.float32, least / len(split), top_value / len(split))
        level = level * jnp.repeat(jnp.exp(draws), shape[dim] // shards_of).reshape((-1,) + (1,) * (len(shape) - 1 - dim))
    return level


def scatter_about(rng, dims, spread, most, shards=(), kind=jnp.bfloat16):
    result = jax.random.normal(rng, dims, jnp.float32) * spread
    if len(shards) > 0:
        result = block_scale(rng, dims, shards, -0.22, 0.18) * result
    return jnp.clip(result, min=-most, max=most).astype(kind)


def setup_inputs(seed: int = 0, part: int = 0) -> dict:
    seeds = jax.random.split(jax.random.key(seed), 8)
    part_keys = jax.random.split(jax.random.fold_in(seeds[7], part), 8)
    hidden = scatter_about(part_keys[0], (TOK, D), 1.0, 6.0, ((1, 8),))
    w_dq = scatter_about(seeds[1], (D, QL), D ** -0.5, 0.0625, ((0, 8),))
    w_dkv = scatter_about(seeds[2], (D, KL + ROPE), D ** -0.5, 0.0625, ((0, 8),))
    q_gain = jnp.clip(1.0 + 0.18 * jax.random.normal(seeds[3], (QL,), jnp.float32), 0.1, 1.9)
    kv_gain = jnp.clip(1.0 + 0.18 * jax.random.normal(seeds[4], (KL,), jnp.float32), 0.1, 1.9)
    w_uq = scatter_about(seeds[5], (QL, HEADS * (NOPE + ROPE)), QL ** -0.5, 0.15625, ((1, 8),))
    w_ukv = scatter_about(seeds[6], (KL, HEADS * (NOPE + VDIM)), KL ** -0.5, 0.25, ((1, 8),))
    return dict(hidden=hidden, w_dq=w_dq, w_dkv=w_dkv, q_gain=q_gain, kv_gain=kv_gain, w_uq=w_uq, w_ukv=w_ukv)


def rotate(values, angle):
    half = values.shape[-1] // 2
    first = values[..., :half]
    second = values[..., half:]
    cosine = jnp.cos(angle)
    sine = jnp.sin(angle)
    return jnp.concatenate([first * cosine - second * sine, second * cosine + first * sine], axis=-1)

def angles(positions, half):
    freqs = 50000.0 ** (-jnp.arange(half, dtype=jnp.float32) / half)
    return positions[:, None] * freqs[None, :]

def normalize(block, gain):
    scale = lax.rsqrt(lax.optimization_barrier(jnp.mean(block * block, axis=1, keepdims=True)) + 1e-06)
    return (block * scale * gain[None, :]).astype(jnp.bfloat16)

def reference(hidden, w_dq, w_dkv, q_gain, kv_gain, w_uq, w_ukv):
    down = jnp.concatenate([jnp.dot(hidden, w_dq, preferred_element_type=jnp.float32), jnp.dot(hidden, w_dkv, preferred_element_type=jnp.float32)], axis=1)
    q_latent = normalize(down[:, :QL], q_gain)
    kv_latent = normalize(down[:, QL:QL + KL], kv_gain)
    positions = jnp.arange(TOK, dtype=jnp.float32)
    angle = angles(positions, ROPE // 2)
    rotary_key = rotate(down[:, QL + KL:], angle).astype(jnp.bfloat16)
    query_full = jnp.dot(q_latent, w_uq, preferred_element_type=jnp.float32)
    query_full = query_full.reshape(TOK, HEADS, NOPE + ROPE)
    turned = rotate(query_full[:, :, NOPE:], angle[:, None, :])
    queries = jnp.concatenate([query_full[:, :, :NOPE], turned], axis=2)
    queries = queries.reshape(TOK, HEADS * (NOPE + ROPE)).astype(jnp.bfloat16)
    keys_values = jnp.dot(kv_latent, w_ukv, preferred_element_type=jnp.float32).astype(jnp.bfloat16)
    return (queries, keys_values, rotary_key)
```

```python
import functools

import jax
import jax.numpy as jnp
from jax import lax
from jax.experimental import pallas as pl
from jax.experimental.pallas import tpu as pltpu
from jax.sharding import PartitionSpec as P


ROPE = 64
CHIPS = 4
ROWS = 128
HALF = ROWS // 2
MIB = 1024 * 1024

VMEM = pltpu.MemorySpace.VMEM
HBM = pltpu.MemorySpace.HBM
F32 = jnp.float32
BF16 = jnp.bfloat16


AHEAD = [(2 * c + k, 2 * ((c + 1 - 2 * k) % CHIPS) + k) for c in range(CHIPS) for k in range(2)]
ACROSS = [(2 * c + k, 2 * ((c + 1 - 2 * k) % CHIPS) + 1 - k) for c in range(CHIPS) for k in range(2)]
SWAP = [(t, t ^ 1) for t in range(2 * CHIPS)]


def send(value, way):
    return lax.ppermute(value, "tensor", way)


def place():
    t = lax.axis_index("tensor")
    return t // 2, t % 2


def block(chip, half):
    return lax.rem(chip + 2 * CHIPS, CHIPS) * 2 + half


def params(mib):
    return pltpu.CompilerParams(vmem_limit_bytes=mib * MIB)


def cost(flops, nbytes):
    return pl.CostEstimate(flops=int(flops), bytes_accessed=int(nbytes), transcendentals=0)


def wanted(group):
    c, k = place()
    ahead, back = c + 1 - 2 * k, c - 1 + 2 * k
    other = [block(c + 2, k), block(back, 1 - k), block(back, k), block(c, 1 - k)]
    mine = [block(c + 2, 1 - k), block(ahead, k), block(ahead, 1 - k), block(c, k)]
    return other[group], mine[group]


def down_kernel(groups, h_ref, wq_ref, wkv_ref, other_ref, mine_ref, x, wq, wkv, ob, mb, sem_x, sem_w, sem_o):
    n = len(groups)
    ql, kv = wq_ref.shape[1], wkv_ref.shape[0]
    reads = []
    for i, group in enumerate(groups):
        for j, b in enumerate(wanted(group)):
            src = h_ref.at[pl.ds(pl.multiple_of(b * ROWS, ROWS), ROWS), :]
            copy = pltpu.make_async_copy(src, x.at[pl.ds((2 * i + j) * ROWS, ROWS), :], sem_x.at[2 * i + j])
            copy.start()
            reads.append(copy)
    loads = []
    for s, lo in enumerate(range(0, ql, 512)):
        copy = pltpu.make_async_copy(wq_ref.at[:, pl.ds(lo, 512)], wq.at[:, pl.ds(lo, 512)], sem_w.at[s])
        copy.start()
        loads.append(copy)
    copy = pltpu.make_async_copy(wkv_ref, wkv, sem_w.at[len(loads)])
    copy.start()
    loads.append(copy)
    for copy in reads:
        copy.wait()

    writes = []

    def emit(lo, hi, y):
        for i in range(n):
            at = i * 2 * ROWS
            ob[i * ROWS : (i + 1) * ROWS, lo:hi] = y[at : at + ROWS].astype(ob.dtype)
            mb[i * ROWS : (i + 1) * ROWS, lo:hi] = y[at + ROWS : at + 2 * ROWS]
        for src, dst, s in ((ob, other_ref, 0), (mb, mine_ref, 1)):
            cols = pl.ds(lo, hi - lo)
            copy = pltpu.make_async_copy(src.at[:, cols], dst.at[:, cols], sem_o.at[2 * (lo // 512) + s])
            copy.start()
            writes.append(copy)

    for s, lo in enumerate(range(0, ql, 512)):
        loads[s].wait()
        emit(lo, lo + 512, jnp.dot(x[...], wq[:, lo : lo + 512], preferred_element_type=F32))
    loads[-1].wait()
    nt = (((1,), (1,)), ((), ()))
    pad = ob.shape[1] - ql - kv

    y = lax.dot_general(x[...], wkv[...], nt, preferred_element_type=F32)
    emit(ql, ql + kv + pad, jnp.concatenate([y, jnp.zeros((2 * n * ROWS, pad), F32)], axis=1))
    for copy in writes:
        copy.wait()


def down(groups, hidden, w_dq, w_dkv_t, dtype):
    n = len(groups)
    depth = hidden.shape[1]
    width = w_dq.shape[1] + w_dkv_t.shape[0]
    width += -width % 128
    return pl.pallas_call(
        functools.partial(down_kernel, groups),
        out_shape=(jax.ShapeDtypeStruct((n * ROWS, width), dtype), jax.ShapeDtypeStruct((n * ROWS, width), F32)),
        in_specs=[pl.BlockSpec(memory_space=HBM)] * 3,
        out_specs=[pl.BlockSpec(memory_space=HBM)] * 2,
        scratch_shapes=[
            pltpu.VMEM((2 * n * ROWS, depth), BF16),
            pltpu.VMEM(w_dq.shape, BF16),
            pltpu.VMEM(w_dkv_t.shape, BF16),
            pltpu.VMEM((n * ROWS, width), dtype),
            pltpu.VMEM((n * ROWS, width), F32),
            pltpu.SemaphoreType.DMA((2 * n,)),
            pltpu.SemaphoreType.DMA((4,)),
            pltpu.SemaphoreType.DMA((8,)),
        ],
        compiler_params=params(60),
        cost_estimate=cost(4 * n * ROWS * depth * width, 5e6),
    )(hidden, w_dq, w_dkv_t)


def join_kernel(spans, size, *refs):
    k = len(spans)
    ins, out, bufs, sem = refs[:k], refs[k], refs[k + 1 : -1], refs[-1]
    width = out.shape[1]
    step = 1024
    copies = []
    for lo in range(0, width, step):
        cols = pl.ds(lo, min(step, width - lo))
        row = []
        for i in range(k):
            src = ins[i].at[pl.ds(spans[i], size), cols]
            copy = pltpu.make_async_copy(src, bufs[i].at[:, cols], sem.at[i, lo // step])
            copy.start()
            row.append(copy)
        copies.append(row)
    for s, lo in enumerate(range(0, width, step)):
        cols = slice(lo, min(lo + step, width))
        for copy in copies[s]:
            copy.wait()
        acc = bufs[0][:, cols].astype(F32)
        for buf in bufs[1:]:
            acc = acc + buf[:, cols].astype(F32)
        out[:, cols] = acc.astype(out.dtype)


def join(size, *parts):
    width = parts[0][0].shape[1]
    return pl.pallas_call(
        functools.partial(join_kernel, [start for _, start in parts], size),
        out_shape=jax.ShapeDtypeStruct((size, width), BF16),
        in_specs=[pl.BlockSpec(memory_space=HBM)] * len(parts),
        out_specs=pl.BlockSpec(memory_space=VMEM),
        scratch_shapes=[pltpu.VMEM((size, width), a.dtype) for a, _ in parts]
        + [pltpu.SemaphoreType.DMA((len(parts), 3))],
        compiler_params=params(8),
        cost_estimate=cost(1e6, 2e6),
    )(*[a for a, _ in parts])


def norm_kernel(spans, size, *refs):
    k = len(spans)
    ins, (qg_ref, kg_ref, lat_ref, rot_ref), bufs, sem = refs[:k], refs[k : k + 4], refs[k + 4 : -1], refs[-1]
    copies = []
    for i in range(k):
        copy = pltpu.make_async_copy(ins[i].at[pl.ds(spans[i], size), :], bufs[i], sem.at[i])
        copy.start()
        copies.append(copy)
    for copy in copies:
        copy.wait()
    ql = qg_ref.shape[1]
    kl = kg_ref.shape[1]

    def total(lo, hi):
        acc = bufs[0][:, lo:hi].astype(F32)
        for buf in bufs[1:]:
            acc = acc + buf[:, lo:hi].astype(F32)
        return acc

    q = total(0, ql)
    scale = lax.rsqrt(jnp.mean(q * q, axis=1, keepdims=True) + 1e-06)
    lat_ref[:, :ql] = (q * scale * qg_ref[...]).astype(BF16)
    v = total(ql, ql + kl)
    scale = lax.rsqrt(jnp.mean(v * v, axis=1, keepdims=True) + 1e-06)
    lat_ref[:, ql : ql + kl] = (v * scale * kg_ref[...]).astype(BF16)
    rot_ref[...] = total(ql + kl, ql + kl + 128)


def norm(size, q_gain, kv_gain, *parts):
    width = q_gain.shape[1] + kv_gain.shape[1]
    full = parts[0][0].shape[1]
    return pl.pallas_call(
        functools.partial(norm_kernel, [start for _, start in parts], size),
        out_shape=(jax.ShapeDtypeStruct((size, width), BF16), jax.ShapeDtypeStruct((size, 128), F32)),
        in_specs=[pl.BlockSpec(memory_space=HBM)] * len(parts) + [pl.BlockSpec(memory_space=VMEM)] * 2,
        out_specs=[pl.BlockSpec(memory_space=VMEM)] * 2,
        scratch_shapes=[pltpu.VMEM((size, full), a.dtype) for a, _ in parts]
        + [pltpu.SemaphoreType.DMA((len(parts),))],
        compiler_params=params(8),
        cost_estimate=cost(2e6, 2e6),
    )(*[a for a, _ in parts], q_gain, kv_gain)


def up_kernel(which, count, *refs):
    mine = refs[:count]
    other = refs[count : 2 * count]
    wq_ref, wkv_ref, cos_ref, sin_ref = refs[2 * count : 2 * count + 4]
    q_out, kv_out, xs, qs, kvs, cos, sin, sem_q, sem_kv = refs[-9:]
    c, k = place()
    ahead, back = c + 1 - 2 * k, c - 1 + 2 * k
    first, second = {
        "own": (block(c, k), block(c, 1 - k)),
        "near": (block(back, k), block(ahead, 1 - k)),
        "late": (block(back, 1 - k), block(ahead, k)),
        "far": (block(c + 2, k), block(c + 2, 1 - k)),
    }[which]
    starts = [pl.multiple_of(b * ROWS, ROWS) for b in (first, second)]
    at = 0
    for piece in (*mine, *other):
        size = piece.shape[0]
        xs[at : at + size, :] = piece[...]
        at += size
    for i, start in enumerate(starts):
        cos[i * ROWS : (i + 1) * ROWS, :] = cos_ref[pl.ds(start, ROWS), :]
        sin[i * ROWS : (i + 1) * ROWS, :] = sin_ref[pl.ds(start, ROWS), :]
    ql = wq_ref.shape[0]
    lane = lax.broadcasted_iota(jnp.int32, (2 * ROWS, 128), 1)
    low = (lane & 32) == 0

    def turn(v, shift):
        cosine, sine = cos[...], sin[...]
        if shift:
            cosine, sine = pltpu.roll(cosine, shift, 1), pltpu.roll(sine, shift, 1)
        partner = jnp.where(low, pltpu.roll(v, 96, 1), pltpu.roll(v, 32, 1))
        return (v * cosine + partner * sine).astype(BF16)

    def out(buf, dst, sem, j, step):
        cols = pl.ds(j * step, step)
        return [
            pltpu.make_async_copy(buf.at[pl.ds(i * ROWS, ROWS), cols], dst.at[pl.ds(start, ROWS), cols], sem.at[2 * j + i])
            for i, start in enumerate(starts)
        ]

    q_step, kv_step = 768, 512
    q_count, kv_count = wq_ref.shape[1] // q_step, wkv_ref.shape[1] // kv_step

    for j in range(q_count):
        lo = j * q_step
        y = jnp.dot(xs[:, :ql], wq_ref[:, lo : lo + q_step], preferred_element_type=F32)
        for g in range(q_step // 384):
            v = y[:, g * 384 : (g + 1) * 384]
            at = lo + g * 384
            qs[:, at : at + 128] = v[:, :128].astype(BF16)
            qs[:, at + 128 : at + 256] = turn(v[:, 128:256], 0)
            qs[:, at + 256 : at + 384] = turn(v[:, 256:], 64)
        for copy in out(qs, q_out, sem_q, j, q_step):
            copy.start()
    for j in range(kv_count):
        cols = slice(j * kv_step, (j + 1) * kv_step)
        kvs[:, cols] = jnp.dot(xs[:, ql:], wkv_ref[:, cols], preferred_element_type=F32).astype(BF16)
        for copy in out(kvs, kv_out, sem_kv, j, kv_step):
            copy.start()
    for j in range(q_count):
        for copy in out(qs, q_out, sem_q, j, q_step):
            copy.wait()
    for j in range(kv_count):
        for copy in out(kvs, kv_out, sem_kv, j, kv_step):
            copy.wait()


def up(which, mine, other, w_uq, w_ukv, cosine, sine, outs):
    tokens = 2 * ROWS * CHIPS
    q_width, kv_width = w_uq.shape[1], w_ukv.shape[1]
    shapes = (jax.ShapeDtypeStruct((tokens, q_width), BF16), jax.ShapeDtypeStruct((tokens, kv_width), BF16))
    args = [*mine, *other, w_uq, w_ukv, cosine, sine]
    specs = [pl.BlockSpec(memory_space=VMEM)] * len(args)
    aliases = {}
    if outs is not None:
        aliases = {len(args): 0, len(args) + 1: 1}
        args += list(outs)
        specs += [pl.BlockSpec(memory_space=HBM)] * 2
    return pl.pallas_call(
        functools.partial(up_kernel, which, len(mine)),
        out_shape=shapes,
        in_specs=specs,
        out_specs=[pl.BlockSpec(memory_space=HBM)] * 2,
        input_output_aliases=aliases,
        scratch_shapes=[
            pltpu.VMEM((2 * ROWS, w_uq.shape[0] + w_ukv.shape[0]), BF16),
            pltpu.VMEM((2 * ROWS, q_width), BF16),
            pltpu.VMEM((2 * ROWS, kv_width), BF16),
            pltpu.VMEM((2 * ROWS, 128), F32),
            pltpu.VMEM((2 * ROWS, 128), F32),
            pltpu.SemaphoreType.DMA((4,)),
            pltpu.SemaphoreType.DMA((8,)),
        ],
        compiler_params=params(24),
        cost_estimate=cost(4 * ROWS * (w_uq.shape[0] * q_width + w_ukv.shape[0] * kv_width), 9e6),
    )(*args)


def angles(first_row, count, half):
    positions = (first_row + lax.iota(jnp.int32, count)).astype(F32)
    freqs = 50000.0 ** (-jnp.arange(half, dtype=F32) / half)
    return positions[:, None] * freqs[None, :]


def rotate(values, angle):
    half = values.shape[-1] // 2
    first = values[..., :half]
    second = values[..., half:]
    cosine = jnp.cos(angle)
    sine = jnp.sin(angle)
    return jnp.concatenate([first * cosine - second * sine, second * cosine + first * sine], axis=-1)


def program(hidden, w_dq, w_dkv, q_gain, kv_gain, w_uq, w_ukv):
    tokens = hidden.shape[0]
    gains = (q_gain[None, :], kv_gain[None, :])
    w_dkv_t = w_dkv.T

    o0, m0 = down((0,), hidden, w_dq, w_dkv_t, F32)
    s0 = send(o0, SWAP)
    hidden, o0 = lax.optimization_barrier((hidden, o0))
    o1, m1 = down((1,), hidden, w_dq, w_dkv_t, F32)
    s1 = send(o1, SWAP)
    a_in = join(ROWS, (m0, 0), (s0, 0))
    a = send(a_in, AHEAD)
    o2, m2 = down((2, 3), hidden, w_dq, w_dkv_t, F32)
    s2 = send(o2, SWAP)
    b_in = join(ROWS, (m1, 0), (s1, 0))
    b = send(b_in, AHEAD)
    c1 = send(join(HALF, (m2, 0), (s2, 0), (a, 0)), ACROSS)
    c2 = send(join(HALF, (m2, HALF), (s2, HALF), (a, HALF)), ACROSS)
    at = ROWS
    lat1, rot1 = norm(HALF, *gains, (m2, at), (s2, at), (b, 0), (c1, 0))
    lat2, rot2 = norm(HALF, *gains, (m2, at + HALF), (s2, at + HALF), (b, HALF), (c2, 0))

    positions, _ = lax.optimization_barrier((lax.iota(jnp.int32, tokens), b_in))
    freqs = 50000.0 ** (-jnp.arange(ROPE // 2, dtype=F32) / (ROPE // 2))
    angle = positions.astype(F32)[:, None] * freqs[None, :]
    cosine, sine = jnp.cos(angle), jnp.sin(angle)
    ones = jnp.ones((tokens, 128 - ROPE), F32)
    cos_table = jnp.concatenate([cosine, cosine, ones], axis=1)
    sin_table = jnp.concatenate([-sine, sine, jnp.zeros_like(ones)], axis=1)
    weights = (w_uq, w_ukv, cos_table, sin_table)

    d1 = send(lat1, AHEAD)
    d2 = send(lat2, AHEAD)
    own = [lat1, lat2]
    swapped = [send(lat1, SWAP), send(lat2, SWAP)]
    d3 = [send(swapped[0], AHEAD), send(swapped[1], AHEAD)]
    far = [send(d1, AHEAD), send(d2, AHEAD)]
    near_swapped = [send(d1, SWAP), send(d2, SWAP)]
    late_swapped = [send(d3[0], SWAP), send(d3[1], SWAP)]
    far_swapped = [send(far[0], SWAP), send(far[1], SWAP)]

    outs = up("own", own, swapped, *weights, None)
    outs = up("near", [d1, d2], near_swapped, *weights, outs)
    outs = up("late", d3, late_swapped, *weights, outs)
    outs = up("far", far, far_swapped, *weights, outs)

    own_start = lax.axis_index("tensor") * ROWS
    raw = jnp.concatenate([rot1, rot2], axis=0)[:, :ROPE]
    rotary_key = rotate(raw, angles(own_start, ROWS, ROPE // 2)).astype(BF16)
    return (*outs, rotary_key)


def solution(mesh):
    in_specs = (
        P("dp", "tensor"),
        P("tensor", None),
        P("tensor", None),
        P(),
        P(),
        P(None, "tensor"),
        P(None, "tensor"),
    )
    out_specs = (P("dp", "tensor"), P("dp", "tensor"), P(("dp", "tensor"), None))
    return jax.shard_map(program, mesh=mesh, in_specs=in_specs, out_specs=out_specs, check_vma=False)
```

```python
import functools

import jax
import jax.numpy as jnp
from jax import lax
from jax.experimental import pallas as pl
from jax.experimental.pallas import tpu as pltpu
from jax.sharding import PartitionSpec as P


ROPE = 64
CHIPS = 4
ROWS = 128
MIB = 1024 * 1024

VMEM = pltpu.MemorySpace.VMEM
HBM = pltpu.MemorySpace.HBM
F32 = jnp.float32
BF16 = jnp.bfloat16
FIRST_LIMIT = 24 * MIB
SWAPPED = F32


AHEAD = [(2 * c + k, 2 * ((c + 1 - 2 * k) % CHIPS) + k) for c in range(CHIPS) for k in range(2)]
ACROSS = [(2 * c + k, 2 * ((c + 1 - 2 * k) % CHIPS) + 1 - k) for c in range(CHIPS) for k in range(2)]
SWAP = [(t, t ^ 1) for t in range(2 * CHIPS)]


def send(value, way):
    return lax.ppermute(value, "tensor", way)


def place():
    t = lax.axis_index("tensor")
    return t // 2, t % 2


def block(chip, half):
    return lax.rem(chip + 2 * CHIPS, CHIPS) * 2 + half


def params(mib):
    return pltpu.CompilerParams(vmem_limit_bytes=mib * MIB)


def cost(flops, nbytes):
    return pl.CostEstimate(flops=int(flops), bytes_accessed=int(nbytes), transcendentals=0)


def wanted(group):
    c, k = place()
    ahead, back = c + 1 - 2 * k, c - 1 + 2 * k
    other = [block(c + 2, k), block(back, 1 - k), block(back, k), block(c, 1 - k)]
    mine = [block(c + 2, 1 - k), block(ahead, k), block(ahead, 1 - k), block(c, k)]
    return other[group], mine[group]


def down_kernel(groups, h_ref, wq_ref, wkv_ref, *outs):
    n = len(groups)
    ql, kv = wq_ref.shape[1], wkv_ref.shape[0]
    blocks = [pl.multiple_of(b * ROWS, ROWS) for group in groups for b in wanted(group)]
    x = jnp.concatenate([h_ref[pl.ds(b, ROWS), :] for b in blocks], axis=0)

    def emit(lo, hi, y):
        row = [0, 0]
        for i in range(2 * n):
            side = i % 2
            at = 0 if row[side] < outs[side].shape[0] else 2
            start = row[side] - (outs[side].shape[0] if at else 0)
            outs[at + side][start : start + ROWS, lo:hi] = y[i * ROWS : (i + 1) * ROWS].astype(outs[at + side].dtype)
            row[side] += ROWS

    for lo in range(0, ql, 512):
        emit(lo, lo + 512, jnp.dot(x, wq_ref[:, lo : lo + 512], preferred_element_type=F32))
    pad = outs[0].shape[1] - ql - kv
    y = lax.dot_general(x, wkv_ref[...], (((1,), (1,)), ((), ())), preferred_element_type=F32)
    emit(ql, ql + kv + pad, jnp.concatenate([y, jnp.zeros((2 * n * ROWS, pad), F32)], axis=1))


def first_kernel(h_ref, wq_ref, wkv_ref, other_ref, mine_ref, h, wq, wkv, sem):
    ql, kv = wq_ref.shape[1], wkv_ref.shape[0]
    blocks = [pl.multiple_of(b * ROWS, ROWS) for b in wanted(0)]
    need = []
    for i, b in enumerate(blocks):
        need.append(pltpu.make_async_copy(h_ref.at[pl.ds(b, ROWS), :], h.at[pl.ds(b, ROWS), :], sem.at[i]))
    loads = []
    for i, lo in enumerate(range(0, ql, 512)):
        cols = pl.ds(lo, 512)
        loads.append(pltpu.make_async_copy(wq_ref.at[:, cols], wq.at[:, cols], sem.at[2 + i]))
    loads.append(pltpu.make_async_copy(wkv_ref, wkv, sem.at[5]))
    rest = []
    for i in range(h_ref.shape[0] // ROWS - 2):
        b = pl.multiple_of(later_block(i) * ROWS, ROWS)
        rest.append(pltpu.make_async_copy(h_ref.at[pl.ds(b, ROWS), :], h.at[pl.ds(b, ROWS), :], sem.at[6 + i]))
    for copy in (*need, *loads, *rest):
        copy.start()
    for copy in need:
        copy.wait()
    x = jnp.concatenate([h[pl.ds(b, ROWS), :] for b in blocks], axis=0)

    def emit(lo, hi, y):
        other_ref[:, lo:hi] = y[:ROWS].astype(other_ref.dtype)
        mine_ref[:, lo:hi] = y[ROWS:]

    for i, lo in enumerate(range(0, ql, 512)):
        loads[i].wait()
        emit(lo, lo + 512, jnp.dot(x, wq[:, lo : lo + 512], preferred_element_type=F32))
    loads[-1].wait()
    pad = other_ref.shape[1] - ql - kv
    y = lax.dot_general(x, wkv[...], (((1,), (1,)), ((), ())), preferred_element_type=F32)
    emit(ql, ql + kv + pad, jnp.concatenate([y, jnp.zeros((2 * ROWS, pad), F32)], axis=1))
    for copy in rest:
        copy.wait()


def later_block(i):
    c, _ = place()
    return block(c + 3 + i // 2, i % 2)


def first(hidden, w_dq, w_dkv_t, dtype):
    width = w_dq.shape[1] + w_dkv_t.shape[0]
    width += -width % 128
    shapes = [jax.ShapeDtypeStruct((ROWS, width), t) for t in (dtype, F32)]
    shapes += [jax.ShapeDtypeStruct(a.shape, a.dtype) for a in (hidden, w_dq, w_dkv_t)]
    return pl.pallas_call(
        first_kernel,
        out_shape=shapes,
        in_specs=[pl.BlockSpec(memory_space=HBM)] * 3,
        out_specs=[pl.BlockSpec(memory_space=VMEM)] * len(shapes),
        scratch_shapes=[pltpu.SemaphoreType.DMA((12,))],
        compiler_params=pltpu.CompilerParams(vmem_limit_bytes=FIRST_LIMIT),
        cost_estimate=cost(4 * ROWS * hidden.shape[1] * width, 5e6),
    )(*[pltpu.with_memory_space_constraint(a, HBM) for a in (hidden, w_dq, w_dkv_t)])


def down(groups, hidden, w_dq, w_dkv_t, dtype):
    n = len(groups)
    depth = hidden.shape[1]
    width = w_dq.shape[1] + w_dkv_t.shape[0]
    width += -width % 128
    shapes = [jax.ShapeDtypeStruct((n * ROWS, width), t) for t in (dtype, F32)]
    return pl.pallas_call(
        functools.partial(down_kernel, groups),
        out_shape=shapes,
        in_specs=[pl.BlockSpec(memory_space=VMEM)] * 3,
        out_specs=[pl.BlockSpec(memory_space=VMEM)] * len(shapes),
        compiler_params=params(24),
        cost_estimate=cost(4 * n * ROWS * depth * width, 5e6),
    )(hidden, w_dq, w_dkv_t)


def join_kernel(spans, *refs):
    ins, out = refs[:-1], refs[-1]
    size = out.shape[0]
    acc = ins[0][spans[0] : spans[0] + size, :].astype(F32)
    for ref, start in zip(ins[1:], spans[1:]):
        acc = acc + ref[start : start + size, :].astype(F32)
    out[...] = acc.astype(out.dtype)


def join(size, *parts):
    width = parts[0][0].shape[1]
    return pl.pallas_call(
        functools.partial(join_kernel, [start for _, start in parts]),
        out_shape=jax.ShapeDtypeStruct((size, width), BF16),
        in_specs=[pl.BlockSpec(memory_space=VMEM)] * len(parts),
        out_specs=pl.BlockSpec(memory_space=VMEM),
        compiler_params=params(16),
        cost_estimate=cost(1e6, 2e6),
    )(*[a for a, _ in parts])


def norm_kernel(spans, *refs):
    ins, (qg_ref, kg_ref, lat_ref, rot_ref) = refs[:-4], refs[-4:]
    size = lat_ref.shape[0]
    ql = qg_ref.shape[1]
    kl = kg_ref.shape[1]

    def total(lo, hi):
        acc = ins[0][spans[0] : spans[0] + size, lo:hi].astype(F32)
        for ref, start in zip(ins[1:], spans[1:]):
            acc = acc + ref[start : start + size, lo:hi].astype(F32)
        return acc

    q = total(0, ql)
    scale = lax.rsqrt(jnp.mean(q * q, axis=1, keepdims=True) + 1e-06)
    lat_ref[:, :ql] = (q * scale * qg_ref[...]).astype(BF16)
    v = total(ql, ql + kl)
    scale = lax.rsqrt(jnp.mean(v * v, axis=1, keepdims=True) + 1e-06)
    lat_ref[:, ql : ql + kl] = (v * scale * kg_ref[...]).astype(BF16)
    rot_ref[...] = total(ql + kl, ql + kl + 128)


def norm(size, q_gain, kv_gain, *parts):
    width = q_gain.shape[1] + kv_gain.shape[1]
    return pl.pallas_call(
        functools.partial(norm_kernel, [start for _, start in parts]),
        out_shape=(jax.ShapeDtypeStruct((size, width), BF16), jax.ShapeDtypeStruct((size, 128), F32)),
        in_specs=[pl.BlockSpec(memory_space=VMEM)] * (len(parts) + 2),
        out_specs=[pl.BlockSpec(memory_space=VMEM)] * 2,
        compiler_params=params(16),
        cost_estimate=cost(2e6, 2e6),
    )(*[a for a, _ in parts], q_gain, kv_gain)


def up_kernel(which, count, *refs):
    pieces = refs[:count]
    wq_ref, wkv_ref, cos_ref, sin_ref = refs[count : count + 4]
    q_out, kv_out, xs, qs, kvs, cos, sin, sem_q, sem_kv = refs[-9:]
    c, k = place()
    ahead, back = c + 1 - 2 * k, c - 1 + 2 * k
    blocks = {
        "own": (block(c, k), block(c, 1 - k)),
        "near": (block(back, k), block(ahead, 1 - k)),
        "late": (block(back, 1 - k), block(ahead, k)),
        "far1": (block(c + 2, k),),
        "far2": (block(c + 2, 1 - k),),
    }[which]
    total = count * ROWS
    starts = [pl.multiple_of(b * ROWS, ROWS) for b in blocks]
    at = 0
    for piece in pieces:
        size = piece.shape[0]
        xs[at : at + size, :] = piece[...]
        at += size
    for i, start in enumerate(starts):
        cos[i * ROWS : (i + 1) * ROWS, :] = cos_ref[pl.ds(start, ROWS), :]
        sin[i * ROWS : (i + 1) * ROWS, :] = sin_ref[pl.ds(start, ROWS), :]
    ql = wq_ref.shape[0]
    lane = lax.broadcasted_iota(jnp.int32, (total, 128), 1)
    low = (lane & 32) == 0

    def turn(v, shift):
        cosine, sine = cos[...], sin[...]
        if shift:
            cosine, sine = pltpu.roll(cosine, shift, 1), pltpu.roll(sine, shift, 1)
        partner = jnp.where(low, pltpu.roll(v, 96, 1), pltpu.roll(v, 32, 1))
        return (v * cosine + partner * sine).astype(BF16)

    def out(buf, dst, sem, j, step):
        cols = pl.ds(j * step, step)
        return [
            pltpu.make_async_copy(buf.at[pl.ds(i * ROWS, ROWS), cols], dst.at[pl.ds(start, ROWS), cols], sem.at[count * j + i])
            for i, start in enumerate(starts)
        ]

    q_step, kv_step = 768, 512
    q_count, kv_count = wq_ref.shape[1] // q_step, wkv_ref.shape[1] // kv_step

    for j in range(q_count):
        lo = j * q_step
        y = jnp.dot(xs[:, :ql], wq_ref[:, lo : lo + q_step], preferred_element_type=F32)
        for g in range(q_step // 384):
            v = y[:, g * 384 : (g + 1) * 384]
            at = lo + g * 384
            qs[:, at : at + 128] = v[:, :128].astype(BF16)
            qs[:, at + 128 : at + 256] = turn(v[:, 128:256], 0)
            qs[:, at + 256 : at + 384] = turn(v[:, 256:], 64)
        for copy in out(qs, q_out, sem_q, j, q_step):
            copy.start()
    for j in range(kv_count):
        cols = slice(j * kv_step, (j + 1) * kv_step)
        kvs[:, cols] = jnp.dot(xs[:, ql:], wkv_ref[:, cols], preferred_element_type=F32).astype(BF16)
        for copy in out(kvs, kv_out, sem_kv, j, kv_step):
            copy.start()
    for j in range(q_count):
        for copy in out(qs, q_out, sem_q, j, q_step):
            copy.wait()
    for j in range(kv_count):
        for copy in out(kvs, kv_out, sem_kv, j, kv_step):
            copy.wait()


def up(which, pieces, w_uq, w_ukv, cosine, sine, outs):
    count = len(pieces)
    tokens = 2 * ROWS * CHIPS
    q_width, kv_width = w_uq.shape[1], w_ukv.shape[1]
    shapes = (jax.ShapeDtypeStruct((tokens, q_width), BF16), jax.ShapeDtypeStruct((tokens, kv_width), BF16))
    args = [*pieces, w_uq, w_ukv, cosine, sine]
    specs = [pl.BlockSpec(memory_space=VMEM)] * len(args)
    aliases = {}
    if outs is not None:
        aliases = {len(args): 0, len(args) + 1: 1}
        args += list(outs)
        specs += [pl.BlockSpec(memory_space=HBM)] * 2
    return pl.pallas_call(
        functools.partial(up_kernel, which, count),
        out_shape=shapes,
        in_specs=specs,
        out_specs=[pl.BlockSpec(memory_space=HBM)] * 2,
        input_output_aliases=aliases,
        scratch_shapes=[
            pltpu.VMEM((count * ROWS, w_uq.shape[0] + w_ukv.shape[0]), BF16),
            pltpu.VMEM((count * ROWS, q_width), BF16),
            pltpu.VMEM((count * ROWS, kv_width), BF16),
            pltpu.VMEM((count * ROWS, 128), F32),
            pltpu.VMEM((count * ROWS, 128), F32),
            pltpu.SemaphoreType.DMA((2 * count,)),
            pltpu.SemaphoreType.DMA((4 * count,)),
        ],
        compiler_params=params(24),
        cost_estimate=cost(2 * count * ROWS * (w_uq.shape[0] * q_width + w_ukv.shape[0] * kv_width), 9e6),
    )(*args)


def rot_kernel(v_ref, cos_ref, sin_ref, out_ref):
    start = pl.multiple_of(lax.axis_index("tensor") * ROWS, ROWS)
    v = v_ref[...]
    lane = lax.broadcasted_iota(jnp.int32, v.shape, 1)
    partner = jnp.where((lane & 32) == 0, pltpu.roll(v, 96, 1), pltpu.roll(v, 32, 1))
    turned = v * cos_ref[pl.ds(start, ROWS), :] + partner * sin_ref[pl.ds(start, ROWS), :]
    out_ref[...] = turned.T[:ROPE].astype(BF16)


def rot(value, cosine, sine):
    return pl.pallas_call(
        rot_kernel,
        out_shape=jax.ShapeDtypeStruct((ROPE, ROWS), BF16),
        in_specs=[pl.BlockSpec(memory_space=VMEM)] * 3,
        out_specs=pl.BlockSpec(memory_space=VMEM),
        compiler_params=params(8),
        cost_estimate=cost(1e5, 1e5),
    )(value, cosine, sine)


def program(hidden, w_dq, w_dkv, q_gain, kv_gain, w_uq, w_ukv):
    tokens = hidden.shape[0]
    gains = (q_gain[None, :], kv_gain[None, :])
    w_dkv_t = w_dkv.T

    o0, m0, hidden, w_dq, w_dkv_t = first(hidden, w_dq, w_dkv_t, BF16)
    s0 = send(o0, SWAP)
    o1, m1 = down((1,), hidden, w_dq, w_dkv_t, SWAPPED)
    s1 = send(o1, SWAP)
    a_in = join(ROWS, (m0, 0), (s0, 0))
    a = send(a_in, AHEAD)
    o2, m2 = down((2, 3), hidden, w_dq, w_dkv_t, SWAPPED)
    s2 = send(o2, SWAP)
    b_in = join(ROWS, (m1, 0), (s1, 0))
    b = send(b_in, AHEAD)
    c = send(join(ROWS, (m2, 0), (s2, 0), (a, 0)), ACROSS)
    lat, raw = norm(ROWS, *gains, (m2, ROWS), (s2, ROWS), (b, 0), (c, 0))

    positions, _ = lax.optimization_barrier((lax.iota(jnp.int32, tokens), a_in))
    freqs = 50000.0 ** (-jnp.arange(ROPE // 2, dtype=F32) / (ROPE // 2))
    angle = positions.astype(F32)[:, None] * freqs[None, :]
    cosine, sine = jnp.cos(angle), jnp.sin(angle)
    ones = jnp.ones((tokens, 128 - ROPE), F32)
    cos_table = jnp.concatenate([cosine, cosine, ones], axis=1)
    sin_table = jnp.concatenate([-sine, sine, jnp.zeros_like(ones)], axis=1)
    weights = (w_uq, w_ukv, cos_table, sin_table)

    near = send(lat, AHEAD)
    swapped = send(lat, SWAP)
    late = send(swapped, AHEAD)
    far = send(near, AHEAD)
    near_swapped = send(near, SWAP)
    late_swapped = send(late, SWAP)
    far_swapped = send(far, SWAP)

    outs = up("own", [lat, swapped], *weights, None)
    outs = up("near", [near, near_swapped], *weights, outs)
    outs = up("late", [late, late_swapped], *weights, outs)
    outs = up("far1", [far], *weights, outs)
    outs = up("far2", [far_swapped], *weights, outs)
    rotary_key = rot(raw, cos_table, sin_table).T
    return (*outs, rotary_key)


def solution(mesh):
    in_specs = (
        P("dp", "tensor"),
        P("tensor", None),
        P("tensor", None),
        P(),
        P(),
        P(None, "tensor"),
        P(None, "tensor"),
    )
    out_specs = (P("dp", "tensor"), P("dp", "tensor"), P(("dp", "tensor"), None))
    return jax.shard_map(program, mesh=mesh, in_specs=in_specs, out_specs=out_specs, check_vma=False)
```

```python
import functools

import jax
import jax.numpy as jnp
from jax import lax
from jax.experimental import pallas as pl
from jax.experimental.pallas import tpu as pltpu
from jax.sharding import PartitionSpec as P


ROPE = 64
CHIPS = 4
ROWS = 128
HALF = ROWS // 2
MIB = 1024 * 1024

VMEM = pltpu.MemorySpace.VMEM
HBM = pltpu.MemorySpace.HBM
F32 = jnp.float32
BF16 = jnp.bfloat16
FIRST_LIMIT = 24 * MIB
SWAPPED = F32


AHEAD = [(2 * c + k, 2 * ((c + 1 - 2 * k) % CHIPS) + k) for c in range(CHIPS) for k in range(2)]
ACROSS = [(2 * c + k, 2 * ((c + 1 - 2 * k) % CHIPS) + 1 - k) for c in range(CHIPS) for k in range(2)]
SWAP = [(t, t ^ 1) for t in range(2 * CHIPS)]


def send(value, way):
    return lax.ppermute(value, "tensor", way)


def place():
    t = lax.axis_index("tensor")
    return t // 2, t % 2


def block(chip, half):
    return lax.rem(chip + 2 * CHIPS, CHIPS) * 2 + half


def packed(width):
    return ROWS * width // 128


def store(ref, base, lo, y):
    for j in range(y.shape[1] // 128):
        at = base + ROWS * (lo // 128 + j)
        ref[at : at + ROWS, :] = y[:, 128 * j : 128 * (j + 1)].astype(ref.dtype)
    if y.shape[1] % 128:
        tail = y[:, y.shape[1] // 128 * 128 :]
        at = base + ROWS * ((lo + y.shape[1]) // 128)
        ref[at : at + HALF, :] = jnp.concatenate([tail[:HALF], tail[HALF:]], axis=1).astype(ref.dtype)


def params(mib):
    return pltpu.CompilerParams(vmem_limit_bytes=mib * MIB)


def cost(flops, nbytes):
    return pl.CostEstimate(flops=int(flops), bytes_accessed=int(nbytes), transcendentals=0)


def wanted(group):
    c, k = place()
    ahead, back = c + 1 - 2 * k, c - 1 + 2 * k
    other = [block(c + 2, k), block(back, 1 - k), block(back, k), block(c, 1 - k)]
    mine = [block(c + 2, 1 - k), block(ahead, k), block(ahead, 1 - k), block(c, k)]
    return other[group], mine[group]


def down_kernel(groups, h_ref, wq_ref, wkv_ref, *outs):
    n = len(groups)
    ql = wq_ref.shape[1]
    blocks = [pl.multiple_of(b * ROWS, ROWS) for group in groups for b in wanted(group)]
    x = jnp.concatenate([h_ref[pl.ds(b, ROWS), :] for b in blocks], axis=0)

    def emit(lo, y):
        for i in range(2 * n):
            ref = outs[i % 2]
            store(ref, i // 2 * (ref.shape[0] // n), lo, y[i * ROWS : (i + 1) * ROWS])

    for lo in range(0, ql, 512):
        emit(lo, jnp.dot(x, wq_ref[:, lo : lo + 512], preferred_element_type=F32))
    emit(ql, lax.dot_general(x, wkv_ref[...], (((1,), (1,)), ((), ())), preferred_element_type=F32))


def first_kernel(h_ref, wq_ref, wkv_ref, other_ref, mine_ref, h, wq, wkv, sem):
    ql = wq_ref.shape[1]
    blocks = [pl.multiple_of(b * ROWS, ROWS) for b in wanted(0)]
    need = []
    for i, b in enumerate(blocks):
        need.append(pltpu.make_async_copy(h_ref.at[pl.ds(b, ROWS), :], h.at[pl.ds(b, ROWS), :], sem.at[i]))
    loads = []
    for i, lo in enumerate(range(0, ql, 512)):
        cols = pl.ds(lo, 512)
        loads.append(pltpu.make_async_copy(wq_ref.at[:, cols], wq.at[:, cols], sem.at[2 + i]))
    loads.append(pltpu.make_async_copy(wkv_ref, wkv, sem.at[5]))
    rest = []
    for i in range(h_ref.shape[0] // ROWS - 2):
        b = pl.multiple_of(later_block(i) * ROWS, ROWS)
        rest.append(pltpu.make_async_copy(h_ref.at[pl.ds(b, ROWS), :], h.at[pl.ds(b, ROWS), :], sem.at[6 + i]))
    for copy in (*need, *loads, *rest):
        copy.start()
    for copy in need:
        copy.wait()
    x = jnp.concatenate([h[pl.ds(b, ROWS), :] for b in blocks], axis=0)

    def emit(lo, y):
        store(other_ref, 0, lo, y[:ROWS])
        store(mine_ref, 0, lo, y[ROWS:])

    for i, lo in enumerate(range(0, ql, 512)):
        loads[i].wait()
        emit(lo, jnp.dot(x, wq[:, lo : lo + 512], preferred_element_type=F32))
    loads[-1].wait()
    emit(ql, lax.dot_general(x, wkv[...], (((1,), (1,)), ((), ())), preferred_element_type=F32))
    for copy in rest:
        copy.wait()


def later_block(i):
    c, _ = place()
    return block(c + 3 + i // 2, i % 2)


def first(hidden, w_dq, w_dkv_t, dtype):
    width = w_dq.shape[1] + w_dkv_t.shape[0]
    shapes = [jax.ShapeDtypeStruct((packed(width), 128), t) for t in (dtype, F32)]
    shapes += [jax.ShapeDtypeStruct(a.shape, a.dtype) for a in (hidden, w_dq, w_dkv_t)]
    return pl.pallas_call(
        first_kernel,
        out_shape=shapes,
        in_specs=[pl.BlockSpec(memory_space=HBM)] * 3,
        out_specs=[pl.BlockSpec(memory_space=VMEM)] * len(shapes),
        scratch_shapes=[pltpu.SemaphoreType.DMA((12,))],
        compiler_params=pltpu.CompilerParams(vmem_limit_bytes=FIRST_LIMIT),
        cost_estimate=cost(4 * ROWS * hidden.shape[1] * width, 5e6),
    )(*[pltpu.with_memory_space_constraint(a, HBM) for a in (hidden, w_dq, w_dkv_t)])


def down(groups, hidden, w_dq, w_dkv_t, dtype):
    n = len(groups)
    depth = hidden.shape[1]
    width = w_dq.shape[1] + w_dkv_t.shape[0]
    shapes = [jax.ShapeDtypeStruct((n * packed(width), 128), t) for t in (dtype, F32)]
    return pl.pallas_call(
        functools.partial(down_kernel, groups),
        out_shape=shapes,
        in_specs=[pl.BlockSpec(memory_space=VMEM)] * 3,
        out_specs=[pl.BlockSpec(memory_space=VMEM)] * len(shapes),
        compiler_params=params(24),
        cost_estimate=cost(4 * n * ROWS * depth * width, 5e6),
    )(hidden, w_dq, w_dkv_t)


def join_kernel(spans, *refs):
    ins, out = refs[:-1], refs[-1]
    size = out.shape[0]
    acc = ins[0][spans[0] : spans[0] + size, :].astype(F32)
    for ref, start in zip(ins[1:], spans[1:]):
        acc = acc + ref[start : start + size, :].astype(F32)
    out[...] = acc.astype(out.dtype)


def join(size, *parts):
    width = parts[0][0].shape[1]
    return pl.pallas_call(
        functools.partial(join_kernel, [start for _, start in parts]),
        out_shape=jax.ShapeDtypeStruct((size, width), BF16),
        in_specs=[pl.BlockSpec(memory_space=VMEM)] * len(parts),
        out_specs=pl.BlockSpec(memory_space=VMEM),
        compiler_params=params(16),
        cost_estimate=cost(1e6, 2e6),
    )(*[a for a, _ in parts])


def norm_kernel(spans, *refs):
    ins, (qg_ref, kg_ref, lat_ref, rot_ref) = refs[:-4], refs[-4:]
    ql = qg_ref.shape[1]
    kl = kg_ref.shape[1]

    def tile(at, count):
        acc = ins[0][spans[0] + at : spans[0] + at + count, :].astype(F32)
        for ref, start in zip(ins[1:], spans[1:]):
            acc = acc + ref[start + at : start + at + count, :].astype(F32)
        return acc

    def total(lo, hi):
        return jnp.concatenate([tile(at, ROWS) for at in range(lo, hi, 128)], axis=1)

    q = total(0, ql)
    scale = lax.rsqrt(jnp.mean(q * q, axis=1, keepdims=True) + 1e-06)
    lat_ref[:, :ql] = (q * scale * qg_ref[...]).astype(BF16)
    v = total(ql, ql + kl)
    scale = lax.rsqrt(jnp.mean(v * v, axis=1, keepdims=True) + 1e-06)
    lat_ref[:, ql : ql + kl] = (v * scale * kg_ref[...]).astype(BF16)
    rot_ref[...] = tile(ql + kl, HALF)


def norm(q_gain, kv_gain, *parts):
    width = q_gain.shape[1] + kv_gain.shape[1]
    return pl.pallas_call(
        functools.partial(norm_kernel, [start for _, start in parts]),
        out_shape=(jax.ShapeDtypeStruct((ROWS, width), BF16), jax.ShapeDtypeStruct((HALF, 128), F32)),
        in_specs=[pl.BlockSpec(memory_space=VMEM)] * (len(parts) + 2),
        out_specs=[pl.BlockSpec(memory_space=VMEM)] * 2,
        compiler_params=params(16),
        cost_estimate=cost(2e6, 2e6),
    )(*[a for a, _ in parts], q_gain, kv_gain)


def up_kernel(which, count, *refs):
    pieces = refs[:count]
    wq_ref, wkv_ref, cos_ref, sin_ref = refs[count : count + 4]
    q_out, kv_out, xs, qs, kvs, cos, sin, sem_q, sem_kv = refs[-9:]
    c, k = place()
    ahead, back = c + 1 - 2 * k, c - 1 + 2 * k
    blocks = {
        "own": (block(c, k), block(c, 1 - k)),
        "near": (block(back, k), block(ahead, 1 - k)),
        "late": (block(back, 1 - k), block(ahead, k)),
        "far1": (block(c + 2, k),),
        "far2": (block(c + 2, 1 - k),),
    }[which]
    total = count * ROWS
    starts = [pl.multiple_of(b * ROWS, ROWS) for b in blocks]
    at = 0
    for piece in pieces:
        size = piece.shape[0]
        xs[at : at + size, :] = piece[...]
        at += size
    for i, start in enumerate(starts):
        cos[i * ROWS : (i + 1) * ROWS, :] = cos_ref[pl.ds(start, ROWS), :]
        sin[i * ROWS : (i + 1) * ROWS, :] = sin_ref[pl.ds(start, ROWS), :]
    ql = wq_ref.shape[0]
    lane = lax.broadcasted_iota(jnp.int32, (total, 128), 1)
    low = (lane & 32) == 0

    def turn(v, shift):
        cosine, sine = cos[...], sin[...]
        if shift:
            cosine, sine = pltpu.roll(cosine, shift, 1), pltpu.roll(sine, shift, 1)
        partner = jnp.where(low, pltpu.roll(v, 96, 1), pltpu.roll(v, 32, 1))
        return (v * cosine + partner * sine).astype(BF16)

    def out(buf, dst, sem, j, step):
        cols = pl.ds(j * step, step)
        return [
            pltpu.make_async_copy(buf.at[pl.ds(i * ROWS, ROWS), cols], dst.at[pl.ds(start, ROWS), cols], sem.at[count * j + i])
            for i, start in enumerate(starts)
        ]

    q_step, kv_step = 768, 512
    q_count, kv_count = wq_ref.shape[1] // q_step, wkv_ref.shape[1] // kv_step

    for j in range(q_count):
        lo = j * q_step
        y = jnp.dot(xs[:, :ql], wq_ref[:, lo : lo + q_step], preferred_element_type=F32)
        for g in range(q_step // 384):
            v = y[:, g * 384 : (g + 1) * 384]
            at = lo + g * 384
            qs[:, at : at + 128] = v[:, :128].astype(BF16)
            qs[:, at + 128 : at + 256] = turn(v[:, 128:256], 0)
            qs[:, at + 256 : at + 384] = turn(v[:, 256:], 64)
        for copy in out(qs, q_out, sem_q, j, q_step):
            copy.start()
    for j in range(kv_count):
        cols = slice(j * kv_step, (j + 1) * kv_step)
        kvs[:, cols] = jnp.dot(xs[:, ql:], wkv_ref[:, cols], preferred_element_type=F32).astype(BF16)
        for copy in out(kvs, kv_out, sem_kv, j, kv_step):
            copy.start()
    for j in range(q_count):
        for copy in out(qs, q_out, sem_q, j, q_step):
            copy.wait()
    for j in range(kv_count):
        for copy in out(kvs, kv_out, sem_kv, j, kv_step):
            copy.wait()


def up(which, pieces, w_uq, w_ukv, cosine, sine, outs):
    count = len(pieces)
    tokens = 2 * ROWS * CHIPS
    q_width, kv_width = w_uq.shape[1], w_ukv.shape[1]
    shapes = (jax.ShapeDtypeStruct((tokens, q_width), BF16), jax.ShapeDtypeStruct((tokens, kv_width), BF16))
    args = [*pieces, w_uq, w_ukv, cosine, sine]
    specs = [pl.BlockSpec(memory_space=VMEM)] * len(args)
    aliases = {}
    if outs is not None:
        aliases = {len(args): 0, len(args) + 1: 1}
        args += list(outs)
        specs += [pl.BlockSpec(memory_space=HBM)] * 2
    return pl.pallas_call(
        functools.partial(up_kernel, which, count),
        out_shape=shapes,
        in_specs=specs,
        out_specs=[pl.BlockSpec(memory_space=HBM)] * 2,
        input_output_aliases=aliases,
        scratch_shapes=[
            pltpu.VMEM((count * ROWS, w_uq.shape[0] + w_ukv.shape[0]), BF16),
            pltpu.VMEM((count * ROWS, q_width), BF16),
            pltpu.VMEM((count * ROWS, kv_width), BF16),
            pltpu.VMEM((count * ROWS, 128), F32),
            pltpu.VMEM((count * ROWS, 128), F32),
            pltpu.SemaphoreType.DMA((2 * count,)),
            pltpu.SemaphoreType.DMA((4 * count,)),
        ],
        compiler_params=params(24),
        cost_estimate=cost(2 * count * ROWS * (w_uq.shape[0] * q_width + w_ukv.shape[0] * kv_width), 9e6),
    )(*args)


def rot_kernel(v_ref, cos_ref, sin_ref, out_ref):
    start = pl.multiple_of(lax.axis_index("tensor") * ROWS, ROWS)
    v = jnp.concatenate([v_ref[...], pltpu.roll(v_ref[...], ROPE, 1)], axis=0)
    lane = lax.broadcasted_iota(jnp.int32, v.shape, 1)
    partner = jnp.where((lane & 32) == 0, pltpu.roll(v, 96, 1), pltpu.roll(v, 32, 1))
    turned = v * cos_ref[pl.ds(start, ROWS), :] + partner * sin_ref[pl.ds(start, ROWS), :]
    out_ref[...] = turned.T[:ROPE].astype(BF16)


def rot(value, cosine, sine):
    return pl.pallas_call(
        rot_kernel,
        out_shape=jax.ShapeDtypeStruct((ROPE, ROWS), BF16),
        in_specs=[pl.BlockSpec(memory_space=VMEM)] * 3,
        out_specs=pl.BlockSpec(memory_space=VMEM),
        compiler_params=params(8),
        cost_estimate=cost(1e5, 1e5),
    )(value, cosine, sine)


def program(hidden, w_dq, w_dkv, q_gain, kv_gain, w_uq, w_ukv):
    tokens = hidden.shape[0]
    gains = (q_gain[None, :], kv_gain[None, :])
    size = packed(w_dq.shape[1] + w_dkv.shape[1])
    w_dkv_t = w_dkv.T

    o0, m0, hidden, w_dq, w_dkv_t = first(hidden, w_dq, w_dkv_t, BF16)
    s0 = send(o0, SWAP)
    o1, m1 = down((1,), hidden, w_dq, w_dkv_t, SWAPPED)
    s1 = send(o1, SWAP)
    a_in = join(size, (m0, 0), (s0, 0))
    a = send(a_in, AHEAD)
    o2, m2 = down((2, 3), hidden, w_dq, w_dkv_t, SWAPPED)
    s2 = send(o2, SWAP)
    b_in = join(size, (m1, 0), (s1, 0))
    b = send(b_in, AHEAD)
    c = send(join(size, (m2, 0), (s2, 0), (a, 0)), ACROSS)
    lat, raw = norm(*gains, (m2, size), (s2, size), (b, 0), (c, 0))

    positions, _ = lax.optimization_barrier((lax.iota(jnp.int32, tokens), a_in))
    freqs = 50000.0 ** (-jnp.arange(ROPE // 2, dtype=F32) / (ROPE // 2))
    angle = positions.astype(F32)[:, None] * freqs[None, :]
    cosine, sine = jnp.cos(angle), jnp.sin(angle)
    ones = jnp.ones((tokens, 128 - ROPE), F32)
    cos_table = jnp.concatenate([cosine, cosine, ones], axis=1)
    sin_table = jnp.concatenate([-sine, sine, jnp.zeros_like(ones)], axis=1)
    weights = (w_uq, w_ukv, cos_table, sin_table)

    near = send(lat, AHEAD)
    swapped = send(lat, SWAP)
    late = send(swapped, AHEAD)
    far = send(near, AHEAD)
    near_swapped = send(near, SWAP)
    late_swapped = send(late, SWAP)
    far_swapped = send(far, SWAP)

    outs = up("own", [lat, swapped], *weights, None)
    outs = up("near", [near, near_swapped], *weights, outs)
    outs = up("late", [late, late_swapped], *weights, outs)
    outs = up("far1", [far], *weights, outs)
    outs = up("far2", [far_swapped], *weights, outs)
    rotary_key = rot(raw, cos_table, sin_table).T
    return (*outs, rotary_key)


def solution(mesh):
    in_specs = (
        P("dp", "tensor"),
        P("tensor", None),
        P("tensor", None),
        P(),
        P(),
        P(None, "tensor"),
        P(None, "tensor"),
    )
    out_specs = (P("dp", "tensor"), P("dp", "tensor"), P(("dp", "tensor"), None))
    return jax.shard_map(program, mesh=mesh, in_specs=in_specs, out_specs=out_specs, check_vma=False)
```
